32 devices in a mesh: cfg: 2 (over x), seq: 16 (over z, y, core).
Axes of the slice: x: 2, y: 2, z: 4, core: 2. Of those that a mesh axis runs over, the one named last changes fastest.
Arguments:
- hidden: bfloat16 [2, 2048, 1920], P('cfg', 'seq'), may hold values from -6 to 6
- modulation: float32 [6, 1920], replicated, may hold values from -3 to 3
- w_qkv: bfloat16 [3, 1920, 1024], replicated, may hold values from -0.125 to 0.125
- q_gain: float32 [64], replicated, may hold values from 1 to 13, as said below
- k_gain: float32 [64], replicated, may hold values from 1 to 13, as said below
- w_out: bfloat16 [1024, 1920], replicated, may hold values from -0.1875 to 0.1875
- text_count: int32 [2], P('cfg'), may hold values from 1 to 226
- block_order: int32 [16], P('seq'), may hold values from 0 to 15, each once
Outputs:
- guided: float32 [2048, 1920], P('seq', 'cfg')
The draws below stay inside these ranges and needn't reach their ends.
Inputs may be any that keep to these rules, and one draw needn't show every extreme that they name: text_count[b] is how many of the 226 text positions of branch b (0 conditional, 1 unconditional) hold prompt tokens; keys at the other text positions are masked. Seq index j holds positions block_order[j] * 128 to block_order[j] * 128 + 127; every block appears once. `q_gain`: one gain for each of the 64 entries of a head, shared by all heads. `k_gain`: one gain for each of the 64 entries of a head, shared by all heads.
All inputs are finite; a program needn't handle non-finite values.
Results may differ from the reference program's by a relative error of at most 0.015.
The reference program's roundings to bfloat16 on the way (of `modded`, `key_bias`, `weights` and `attended`) count: a program that leaves them out, or rounds other values in their place, can miss the bound.
Values may be sent and summed in bfloat16 or wider, within the bound.
A program may use at most 256 MiB of HBM per device.

```python
import math
import jax
import jax.numpy as jnp
from jax import lax

D = 1920
HEAD = 64
HEADS = 16
TOK_DEV = 128
TXT = 226
TOKENS = 2048
N_SEQ = 16


def norm_gain(key, member):
    large_count = 3
    large_low = 7.0
    large_high = 9.0
    ranking = jax.random.permutation(jax.random.fold_in(key, 9001), HEAD)
    chosen = ranking < large_count
    member_key = jax.random.fold_in(key, member)
    base_gain = jnp.exp(jax.random.uniform(jax.random.fold_in(member_key, 1), (HEAD,), jnp.float32, 0.0, math.log(2.2)))
    large_gain = jax.random.uniform(jax.random.fold_in(member_key, 2), (HEAD,), jnp.float32, large_low, large_high)
    return jnp.where(chosen, large_gain, base_gain).astype(jnp.float32)


def draw_q_gain(key, part):
    return norm_gain(key, 11)


def draw_k_gain(key, part):
    return norm_gain(key, 23)


def steps_of(rng, extent, cuts, smallest, high):
    loudness, own = 1.0, jax.random.fold_in(rng, 6)
    for dim, parts in cuts:
        heights = jnp.exp(jax.random.uniform(jax.random.fold_in(own, dim), (parts,), jnp.float32, smallest / len(cuts), high / len(cuts)))
        loudness = loudness * jnp.repeat(heights, extent[dim] // parts).reshape([-1 if axis == dim else 1 for axis in range(len(extent))])
    return loudness


def gaussian(key, dims, scale, most, split=(), kind=jnp.bfloat16):
    loudness = steps_of(key, dims, split, -0.22, 0.18) if split else 1.0
    drawn = jax.random.normal(key, dims, jnp.float32) * scale * loudness
    return jnp.minimum(jnp.maximum(drawn, -most), most).astype(kind)


def setup_inputs(seed: int = 0) -> dict:
    key_list = jax.random.split(jax.random.key(seed), 9)
    return {
        "hidden": gaussian(key_list[0], (2, TOKENS, D), 1.0, 6.0, ((0, 2), (1, 16))),
        "modulation": gaussian(key_list[1], (6, D), 0.5, 3.0, (), jnp.float32),
        "w_qkv": gaussian(key_list[2], (3, D, HEADS * HEAD), D ** -0.5, 0.125),
        "q_gain": draw_q_gain(jax.random.fold_in(key_list[8], 71), 0),
        "k_gain": draw_k_gain(jax.random.fold_in(key_list[8], 71), 0),
        "w_out": gaussian(key_list[5], (HEADS * HEAD, D), (HEADS * HEAD) ** -0.5, 0.1875),
        "text_count": jax.random.randint(key_list[6], (2,), 1, TXT + 1).astype(jnp.int32),
        "block_order": jax.random.permutation(key_list[7], N_SEQ).astype(jnp.int32),
    }


GUIDANCE = 6.0
EPSILON = 1e-05
MASKED = -1000000000.0

def layer_normal(values_in):
    average = lax.optimization_barrier(jnp.mean(values_in, axis=-1, keepdims=True))
    centred = values_in - average
    spread = lax.optimization_barrier(jnp.mean(centred * centred, axis=-1, keepdims=True))
    return centred * lax.rsqrt(spread + EPSILON)

def modulated(states, is_text, modulation):
    normed = layer_normal(states.astype(jnp.float32))
    shift = jnp.where(is_text[:, None], modulation[3][None, :], modulation[0][None, :])
    scale = jnp.where(is_text[:, None], modulation[4][None, :], modulation[1][None, :])
    return (normed * (1.0 + scale) + shift).astype(jnp.bfloat16)

def head_normal(projected, gain):
    rows = projected.shape[0]
    heads_view = projected.reshape(rows, HEADS, HEAD)
    return (layer_normal(heads_view) * gain).reshape(rows, HEADS * HEAD).astype(jnp.bfloat16)

def projections(states, is_text, modulation, w_qkv, q_gain, k_gain):
    modded = modulated(states, is_text, modulation)
    query = head_normal(jnp.dot(modded, w_qkv[0], preferred_element_type=jnp.float32), q_gain)
    keys = head_normal(jnp.dot(modded, w_qkv[1], preferred_element_type=jnp.float32), k_gain)
    values = jnp.dot(modded, w_qkv[2], preferred_element_type=jnp.float32).astype(jnp.bfloat16)
    return (query, keys, values)

def attend_block(query_block, key_heads, value_heads, bias_wide):
    rows = query_block.shape[0]
    query_heads = query_block.astype(jnp.float32).reshape(rows, HEADS, HEAD)
    scores = jnp.einsum('qhd,khd->hqk', query_heads, key_heads) * HEAD ** (-0.5) + bias_wide[None, None, :]
    highest = lax.optimization_barrier(jnp.max(scores, axis=-1, keepdims=True))
    expo = jnp.exp(scores - highest)
    total = lax.optimization_barrier(jnp.sum(expo, axis=-1))
    weights = expo.astype(jnp.bfloat16).astype(jnp.float32)
    numer = jnp.einsum('hqk,khd->qhd', weights, value_heads)
    return (numer / total.T[:, :, None]).reshape(rows, HEADS * HEAD).astype(jnp.bfloat16)

def reference(hidden, modulation, w_qkv, q_gain, k_gain, w_out, text_count, block_order):
    within = jnp.arange(TOK_DEV, dtype=jnp.int32)
    position = (block_order[:, None].astype(jnp.int32) * TOK_DEV + within[None, :]).reshape(TOKENS)
    is_text = position < TXT
    gate = jnp.where(is_text[:, None], modulation[5][None, :], modulation[2][None, :])
    query_rows = 512 if TOKENS % 512 == 0 else TOKENS

    def one_branch(states, count):
        keep = jnp.logical_or(position >= TXT, position < count)
        key_bias = jnp.where(keep, 0.0, MASKED).astype(jnp.bfloat16)
        query, keys, values = projections(states, is_text, modulation, w_qkv, q_gain, k_gain)
        key_heads = keys.astype(jnp.float32).reshape(TOKENS, HEADS, HEAD)
        value_heads = values.astype(jnp.float32).reshape(TOKENS, HEADS, HEAD)
        bias_wide = key_bias.astype(jnp.float32)
        query_blocks = query.reshape(TOKENS // query_rows, query_rows, HEADS * HEAD)

        def attend(block):
            return attend_block(block, key_heads, value_heads, bias_wide)
        attended = lax.map(attend, query_blocks).reshape(TOKENS, HEADS * HEAD)
        return gate * jnp.dot(attended, w_out, preferred_element_type=jnp.float32)
    cond = one_branch(hidden[0], text_count[0])
    uncond = one_branch(hidden[1], text_count[1])
    return uncond + GUIDANCE * (cond - uncond)
```

```python
import functools

import jax
import jax.numpy as jnp
from jax import lax
from jax.experimental import pallas as pl
from jax.experimental.pallas import tpu as pltpu
from jax.sharding import PartitionSpec as P

HEAD = 64
HEADS = 16
TXT = 226


GUIDANCE = 6.0
EPSILON = 1e-05
MASKED = -1000000000.0


def swapped(block, axis, apart):
    count = lax.axis_size(axis)
    route = []
    for low in range(count):
        high = low | 1 << apart
        if high != low and high < count:
            route += [(low, high), (high, low)]
    return lax.ppermute(block, axis, route)


def layer_normal(values_in):
    average = jnp.mean(values_in, axis=-1, keepdims=True)
    centred = values_in - average
    spread = jnp.mean(centred * centred, axis=-1, keepdims=True)
    return centred * lax.rsqrt(spread + EPSILON)


def modulated(states, is_text, modulation):
    normed = layer_normal(states.astype(jnp.float32))
    shift = jnp.where(is_text[:, None], modulation[3][None, :], modulation[0][None, :])
    scale = jnp.where(is_text[:, None], modulation[4][None, :], modulation[1][None, :])
    return (normed * (1.0 + scale) + shift).astype(jnp.bfloat16)


def head_normal(projected, gain):
    rows = projected.shape[0]
    heads_view = projected.reshape(rows, HEADS, HEAD)
    return (layer_normal(heads_view) * gain).reshape(rows, HEADS * HEAD).astype(jnp.bfloat16)


def projections(states, is_text, modulation, w_qkv, q_gain, k_gain):
    modded = modulated(states, is_text, modulation)
    query = head_normal(jnp.dot(modded, w_qkv[0], preferred_element_type=jnp.float32), q_gain)
    keys = head_normal(jnp.dot(modded, w_qkv[1], preferred_element_type=jnp.float32), k_gain)
    values = jnp.dot(modded, w_qkv[2], preferred_element_type=jnp.float32).astype(jnp.bfloat16)
    return (query, keys, values)


def fold_block(query_heads, carry, piece):
    highest, total, numer = carry
    keys_piece, values_piece, bias_piece = piece
    count = keys_piece.shape[0]
    key_heads = keys_piece.reshape(count, HEADS, HEAD)
    value_heads = values_piece.reshape(count, HEADS, HEAD)
    scores = jnp.einsum("qhd,khd->hqk", query_heads, key_heads, preferred_element_type=jnp.float32)
    scores = scores * HEAD ** (-0.5) + bias_piece.astype(jnp.float32)[None, None, :]
    new_high = jnp.maximum(highest, jnp.max(scores, axis=-1))
    expo = jnp.exp(scores - new_high[:, :, None])
    rescale = jnp.exp(highest - new_high)
    total = jnp.sum(expo, axis=-1)
    numer = numer * rescale.T[:, :, None] + jnp.einsum(
        "hqk,khd->qhd", expo.astype(jnp.bfloat16), value_heads, preferred_element_type=jnp.float32
    )
    return (new_high, total, numer)


def shards(hidden, modulation, w_qkv, q_gain, k_gain, w_out, text_count, block_order):
    states = hidden[0]
    tok_rows = states.shape[0]
    within = jnp.arange(tok_rows, dtype=jnp.int32)
    position = block_order[0] * tok_rows + within
    is_text = position < TXT
    keep = jnp.logical_or(position >= TXT, position < text_count[0])
    key_bias = jnp.where(keep, 0.0, MASKED).astype(jnp.bfloat16)
    query, keys, values = projections(states, is_text, modulation, w_qkv, q_gain, k_gain)
    query_heads = query.reshape(tok_rows, HEADS, HEAD)
    start_state = (
        jnp.full((HEADS, tok_rows), -1e30, jnp.float32),
        jnp.zeros((HEADS, tok_rows), jnp.float32),
        jnp.zeros((tok_rows, HEADS, HEAD), jnp.float32),
    )
    carry = fold_block(
        query_heads,
        start_state,
        (
            lax.all_gather(keys, "seq", axis=0, tiled=True),
            lax.all_gather(values, "seq", axis=0, tiled=True),
            lax.all_gather(key_bias, "seq", axis=0, tiled=True),
        ),
    )
    highest, total, numer = carry
    attended = (numer / total.T[:, :, None]).reshape(tok_rows, HEADS * HEAD).astype(jnp.bfloat16)
    gate = jnp.where(is_text[:, None], modulation[5][None, :], modulation[2][None, :])
    cfg_index = lax.axis_index("cfg")
    half_width = w_out.shape[1] // 2
    w_half = lax.dynamic_slice_in_dim(w_out, cfg_index * half_width, half_width, 1)
    gate_half = lax.dynamic_slice_in_dim(gate, cfg_index * half_width, half_width, 1)
    partner = swapped(attended, "cfg", 0)
    own_update = gate_half * jnp.dot(attended, w_half, preferred_element_type=jnp.float32)
    other_update = gate_half * jnp.dot(partner, w_half, preferred_element_type=jnp.float32)
    is_first = cfg_index == 0
    cond = jnp.where(is_first, own_update, other_update)
    uncond = jnp.where(is_first, other_update, own_update)
    return uncond + GUIDANCE * (cond - uncond)


LANES = 128
GROUPS = 4
MESH = pl.DeviceIdType.MESH


def flip(bit, other):
    return lax.rem(bit + other, 2)


def pair_normal(x, low):
    def halves(y):
        first = jnp.sum(jnp.where(low, y, 0.0), axis=-1, keepdims=True)
        second = jnp.sum(jnp.where(low, 0.0, y), axis=-1, keepdims=True)
        return jnp.where(low, first, second) * (1.0 / HEAD)

    centred = x - halves(x)
    return centred * lax.rsqrt(halves(centred * centred) + EPSILON)


def turned(x):
    return pltpu.roll(x, HEAD, 1)


def fused(n, count_ref, block_ref, hidden_ref, mod_ref, w_ref, qg_ref, kg_ref, wo_ref, out_ref,
          w_buf, wo_buf, modded, kv_out, kv_in, q_out, q_in, bias_out, bias_in, bias_row,
          att_out, att_in, att_far, stacked,
          w_sem, wo_sem, kv_s, kv_r, q_s, q_r, b_s, b_r, a_s, a_r, f_s, f_r):
    me = lax.axis_index("seq")
    cfg = lax.axis_index("cfg")
    rows, width = hidden_ref.shape
    half_rows = rows // 2
    half = width // 2
    wide = wo_buf.shape[1]
    cols = w_buf.shape[3]
    heads_here = cols // HEAD
    plane = lax.div(me, GROUPS)
    plane_high, plane_low = lax.div(plane, 2), lax.rem(plane, 2)

    def group(i):
        high = 1 - lax.div(i, 2)
        lowbit = flip(lax.div(i, 2), lax.rem(i, 2))
        return 2 * flip(plane_high, high) + flip(plane_low, lowbit)

    def weight(kind, i):
        start = pl.multiple_of(group(i) * cols, cols)
        return pltpu.make_async_copy(
            w_ref.at[kind, :, pl.ds(start, cols)], w_buf.at[kind, i], w_sem.at[kind, i])

    column = pl.multiple_of(cfg * (width - wide), LANES)
    out_weight = pltpu.make_async_copy(wo_ref.at[:, pl.ds(column, wide)], wo_buf, wo_sem)

    barrier = pltpu.get_barrier_semaphore()
    for j in range(1, n):
        pl.semaphore_signal(barrier, inc=1, device_id={"seq": lax.rem(me + j, n)}, device_id_type=MESH)
    pl.semaphore_signal(barrier, inc=1, device_id={"cfg": 1 - cfg}, device_id_type=MESH)
    for i in range(GROUPS):
        weight(1, i).start()
        weight(2, i).start()
    for i in range(GROUPS):
        weight(0, i).start()
    out_weight.start()

    def send(src, dst, to, s_sem, r_sem):
        @pl.when(to != me)
        def _():
            pltpu.make_async_remote_copy(
                src_ref=src.at[to], dst_ref=dst.at[me], send_sem=s_sem.at[to], recv_sem=r_sem.at[me],
                device_id={"seq": to}, device_id_type=MESH).start()

        @pl.when(to == me)
        def _():
            pltpu.make_async_copy(src.at[to], dst.at[me], r_sem.at[me]).start()

    def arrived(dst, source, r_sem):
        pltpu.make_async_copy(dst.at[source], dst.at[source], r_sem.at[source]).wait()

    def sent(src, to, s_sem):
        @pl.when(to != me)
        def _():
            pltpu.make_async_copy(src.at[to], src.at[to], s_sem.at[to]).wait()

    block = block_ref[0]
    count = count_ref[0]
    across = block * rows + lax.broadcasted_iota(jnp.int32, (1, rows), 1)
    keep = jnp.logical_or(across >= TXT, across < count)
    bias_out[0:n] = jnp.broadcast_to(jnp.where(keep, 0.0, MASKED)[None], (n, 1, rows)).astype(jnp.bfloat16).astype(jnp.float32)

    mod = mod_ref[...]
    down = block * rows + lax.broadcasted_iota(jnp.int32, (rows, 1), 0)
    is_text = down < TXT
    normed = layer_normal(hidden_ref[...].astype(jnp.float32))
    shift = jnp.where(is_text, mod[3:4, :], mod[0:1, :])
    scale = jnp.where(is_text, mod[4:5, :], mod[1:2, :])
    modded[...] = (normed * (1.0 + scale) + shift).astype(jnp.bfloat16)

    low = lax.broadcasted_iota(jnp.int32, (1, LANES), 1) < HEAD
    pl.semaphore_wait(barrier, n)

    def send_bias(j, carry):
        send(bias_out, bias_in, j, b_s, b_r)
        return carry

    lax.fori_loop(0, n, send_bias, 0)

    k_gain = kg_ref[...]
    q_gain = qg_ref[...] * HEAD ** (-0.5)

    def project_kv(i, carry):
        weight(1, i).wait()
        weight(2, i).wait()
        first = group(i) * heads_here
        x = modded[...]
        k_all = jnp.dot(x, w_buf[1, i], preferred_element_type=jnp.float32)
        v_all = jnp.dot(x, w_buf[2, i], preferred_element_type=jnp.float32)
        for p in range(heads_here // 2):
            k = pair_normal(k_all[:, p * LANES:(p + 1) * LANES], low) * k_gain
            v = v_all[:, p * LANES:(p + 1) * LANES]
            kv_out[first + 2 * p] = jnp.where(low, k, turned(v)).astype(jnp.bfloat16)
            kv_out[first + 2 * p + 1] = jnp.where(low, turned(k), v).astype(jnp.bfloat16)
        for h in range(heads_here):
            send(kv_out, kv_in, first + h, kv_s, kv_r)
        return carry

    lax.fori_loop(0, GROUPS, project_kv, 0)

    def project_q(i, carry):
        weight(0, i).wait()
        first = group(i) * heads_here
        q_all = jnp.dot(modded[...], w_buf[0, i], preferred_element_type=jnp.float32)
        for p in range(heads_here // 2):
            q = pair_normal(q_all[:, p * LANES:(p + 1) * LANES], low) * q_gain
            top, bottom = q[:half_rows], q[half_rows:]
            q_out[first + 2 * p] = jnp.where(low, top, turned(bottom)).astype(jnp.bfloat16)
            q_out[first + 2 * p + 1] = jnp.where(low, turned(top), bottom).astype(jnp.bfloat16)
        for h in range(heads_here):
            send(q_out, q_in, first + h, q_s, q_r)
        return carry

    lax.fori_loop(0, GROUPS, project_q, 0)

    for j in range(n):
        arrived(bias_in, j, b_r)
    for j in range(n):
        bias_row[:, j * rows:(j + 1) * rows] = jnp.broadcast_to(bias_in[j], (8, rows))

    def wait_kv(j, carry):
        arrived(kv_in, j, kv_r)
        return carry

    lax.fori_loop(0, n, wait_kv, 0)

    chip = lax.div(me, 2)

    def pair_of(k):
        c0, c1, c2 = lax.rem(chip, 2), lax.rem(lax.div(chip, 2), 2), lax.div(chip, 4)
        k0, k1, k2 = lax.rem(k, 2), lax.rem(lax.div(k, 2), 2), lax.div(k, 4)
        return 4 * flip(c2, k2) + 2 * flip(c1, k1) + flip(c0, k0)

    def forward(k):
        for i in range(2):
            h = 2 * pair_of(k) + i
            arrived(att_in, h, a_r)
            pltpu.make_async_remote_copy(
                src_ref=att_in.at[h], dst_ref=att_far.at[h], send_sem=f_s.at[h], recv_sem=f_r.at[h],
                device_id={"cfg": 1 - cfg}, device_id_type=MESH).start()

    def attend(k, carry):
        base = 2 * pair_of(k)
        parts = []
        for i in range(2):
            arrived(q_in, base + i, q_r)
            folded = q_in[base + i].astype(jnp.float32)
            parts += [jnp.where(low, folded, 0.0), jnp.where(low, turned(folded), 0.0)]
        query = jnp.concatenate(parts, axis=0).astype(jnp.bfloat16)
        keys = kv_in[...].reshape(n * rows, LANES)
        scores = lax.dot_general(query, keys, (((1,), (1,)), ((), ())), preferred_element_type=jnp.float32)
        scores = scores + bias_row[0:1, :]
        expo = jnp.exp(scores - jnp.max(scores, axis=-1, keepdims=True))
        total = jnp.sum(expo, axis=-1, keepdims=True)
        numer = jnp.dot(expo.astype(jnp.bfloat16), keys, preferred_element_type=jnp.float32)
        result = numer / total
        for i in range(2):
            top = result[i * rows:i * rows + half_rows]
            bottom = result[i * rows + half_rows:(i + 1) * rows]
            att_out[base + i] = jnp.where(low, turned(top), bottom).astype(jnp.bfloat16)
            send(att_out, att_in, base + i, a_s, a_r)

        @pl.when(k >= 2)
        def _():
            forward(k - 2)

        return carry

    steps = n // 2
    lax.fori_loop(0, steps, attend, 0)
    forward(steps - 2)
    forward(steps - 1)
    out_weight.wait()

    def assemble(source, at):
        for p in range(n // 2):
            a = source[2 * p].astype(jnp.float32)
            b = source[2 * p + 1].astype(jnp.float32)
            span = slice(p * LANES, (p + 1) * LANES)
            stacked[at:at + half_rows, span] = jnp.where(low, a, turned(b)).astype(jnp.bfloat16)
            stacked[at + half_rows:at + rows, span] = jnp.where(low, turned(a), b).astype(jnp.bfloat16)

    assemble(att_in, 0)
    for h in range(n):
        arrived(att_far, h, f_r)
    assemble(att_far, rows)
    both = jnp.dot(stacked[...], wo_buf[...], preferred_element_type=jnp.float32)
    is_first = cfg == 0
    gate_text = jnp.where(is_first, mod[5:6, :wide], mod[5:6, width - wide:])
    gate_video = jnp.where(is_first, mod[2:3, :wide], mod[2:3, width - wide:])
    gate = jnp.where(is_text, gate_text, gate_video)
    own, other = gate * both[:rows], gate * both[rows:]
    cond = jnp.where(is_first, own, other)
    uncond = jnp.where(is_first, other, own)
    guided = uncond + GUIDANCE * (cond - uncond)
    excess = wide - half
    guided = jnp.where(is_first, guided, pltpu.roll(guided, half, 1)) if excess else guided
    out_ref[...] = guided[:, :half]

    def finish(j, carry):
        sent(bias_out, j, b_s)
        sent(kv_out, j, kv_s)
        sent(q_out, j, q_s)
        sent(att_out, j, a_s)
        pltpu.make_async_copy(att_in.at[j], att_in.at[j], f_s.at[j]).wait()
        return carry

    lax.fori_loop(0, n, finish, 0)


def whole_kernel(hidden, modulation, w_qkv, q_gain, k_gain, w_out, text_count, block_order):
    n = lax.axis_size("seq")
    states = hidden[0]
    rows, width = states.shape
    features = w_out.shape[0]
    cols = features // GROUPS
    half = width // 2
    wide = -(-half // LANES) * LANES
    bf, f32 = jnp.bfloat16, jnp.float32
    vmem = pl.BlockSpec(memory_space=pltpu.VMEM)
    smem = pl.BlockSpec(memory_space=pltpu.SMEM)
    hbm = pl.BlockSpec(memory_space=pl.ANY)
    dma = pltpu.SemaphoreType.DMA
    double = lambda gain: jnp.concatenate([gain, gain])[None, :]
    return pl.pallas_call(
        functools.partial(fused, n),
        out_shape=jax.ShapeDtypeStruct((rows, half), f32),
        in_specs=[smem, smem, vmem, vmem, hbm, vmem, vmem, hbm],
        out_specs=vmem,
        scratch_shapes=[
            pltpu.VMEM((3, GROUPS, width, cols), bf),
            pltpu.VMEM((features, wide), bf),
            pltpu.VMEM((rows, width), bf),
            pltpu.VMEM((n, rows, LANES), bf),
            pltpu.VMEM((n, rows, LANES), bf),
            pltpu.VMEM((n, rows // 2, LANES), bf),
            pltpu.VMEM((n, rows // 2, LANES), bf),
            pltpu.VMEM((n + 8, 1, rows), f32),
            pltpu.VMEM((n + 8, 1, rows), f32),
            pltpu.VMEM((8, n * rows), f32),
            pltpu.VMEM((n, rows // 2, LANES), bf),
            pltpu.VMEM((n, rows // 2, LANES), bf),
            pltpu.VMEM((n, rows // 2, LANES), bf),
            pltpu.VMEM((2 * rows, features), bf),
            dma((3, GROUPS)),
            dma,
        ] + [dma((n,))] * 10,
        compiler_params=pltpu.CompilerParams(
            collective_id=0, has_side_effects=True, vmem_limit_bytes=60 * 1024 * 1024),
    )(text_count, block_order, states, modulation, w_qkv, double(q_gain), double(k_gain), w_out)


def solution(mesh):
    in_specs = (P("cfg", "seq", None), P(), P(), P(), P(), P(), P("cfg"), P("seq"))
    out_specs = P("seq", "cfg")
    one_head_each = mesh.shape["seq"] == HEADS and mesh.shape["cfg"] == 2
    body = whole_kernel if one_head_each else shards
    return jax.shard_map(body, mesh=mesh, in_specs=in_specs, out_specs=out_specs, check_vma=False)
```

```python
import functools

import jax
import jax.numpy as jnp
from jax import lax
from jax.experimental import pallas as pl
from jax.experimental.pallas import tpu as pltpu
from jax.sharding import PartitionSpec as P

HEAD = 64
HEADS = 16
TXT = 226


GUIDANCE = 6.0
EPSILON = 1e-05
MASKED = -1000000000.0


def swapped(block, axis, apart):
    count = lax.axis_size(axis)
    route = []
    for low in range(count):
        high = low | 1 << apart
        if high != low and high < count:
            route += [(low, high), (high, low)]
    return lax.ppermute(block, axis, route)


def layer_normal(values_in):
    average = jnp.mean(values_in, axis=-1, keepdims=True)
    centred = values_in - average
    spread = jnp.mean(centred * centred, axis=-1, keepdims=True)
    return centred * lax.rsqrt(spread + EPSILON)


def modulated(states, is_text, modulation):
    normed = layer_normal(states.astype(jnp.float32))
    shift = jnp.where(is_text[:, None], modulation[3][None, :], modulation[0][None, :])
    scale = jnp.where(is_text[:, None], modulation[4][None, :], modulation[1][None, :])
    return (normed * (1.0 + scale) + shift).astype(jnp.bfloat16)


def head_normal(projected, gain):
    rows = projected.shape[0]
    heads_view = projected.reshape(rows, HEADS, HEAD)
    return (layer_normal(heads_view) * gain).reshape(rows, HEADS * HEAD).astype(jnp.bfloat16)


def projections(states, is_text, modulation, w_qkv, q_gain, k_gain):
    modded = modulated(states, is_text, modulation)
    query = head_normal(jnp.dot(modded, w_qkv[0], preferred_element_type=jnp.float32), q_gain)
    keys = head_normal(jnp.dot(modded, w_qkv[1], preferred_element_type=jnp.float32), k_gain)
    values = jnp.dot(modded, w_qkv[2], preferred_element_type=jnp.float32).astype(jnp.bfloat16)
    return (query, keys, values)


def fold_block(query_heads, carry, piece):
    highest, total, numer = carry
    keys_piece, values_piece, bias_piece = piece
    count = keys_piece.shape[0]
    key_heads = keys_piece.reshape(count, HEADS, HEAD)
    value_heads = values_piece.reshape(count, HEADS, HEAD)
    scores = jnp.einsum("qhd,khd->hqk", query_heads, key_heads, preferred_element_type=jnp.float32)
    scores = scores * HEAD ** (-0.5) + bias_piece.astype(jnp.float32)[None, None, :]
    new_high = jnp.maximum(highest, jnp.max(scores, axis=-1))
    expo = jnp.exp(scores - new_high[:, :, None])
    rescale = jnp.exp(highest - new_high)
    total = jnp.sum(expo, axis=-1)
    numer = numer * rescale.T[:, :, None] + jnp.einsum(
        "hqk,khd->qhd", expo.astype(jnp.bfloat16), value_heads, preferred_element_type=jnp.float32
    )
    return (new_high, total, numer)


def shards(hidden, modulation, w_qkv, q_gain, k_gain, w_out, text_count, block_order):
    states = hidden[0]
    tok_rows = states.shape[0]
    within = jnp.arange(tok_rows, dtype=jnp.int32)
    position = block_order[0] * tok_rows + within
    is_text = position < TXT
    keep = jnp.logical_or(position >= TXT, position < text_count[0])
    key_bias = jnp.where(keep, 0.0, MASKED).astype(jnp.bfloat16)
    query, keys, values = projections(states, is_text, modulation, w_qkv, q_gain, k_gain)
    query_heads = query.reshape(tok_rows, HEADS, HEAD)
    start_state = (
        jnp.full((HEADS, tok_rows), -1e30, jnp.float32),
        jnp.zeros((HEADS, tok_rows), jnp.float32),
        jnp.zeros((tok_rows, HEADS, HEAD), jnp.float32),
    )
    carry = fold_block(
        query_heads,
        start_state,
        (
            lax.all_gather(keys, "seq", axis=0, tiled=True),
            lax.all_gather(values, "seq", axis=0, tiled=True),
            lax.all_gather(key_bias, "seq", axis=0, tiled=True),
        ),
    )
    highest, total, numer = carry
    attended = (numer / total.T[:, :, None]).reshape(tok_rows, HEADS * HEAD).astype(jnp.bfloat16)
    gate = jnp.where(is_text[:, None], modulation[5][None, :], modulation[2][None, :])
    cfg_index = lax.axis_index("cfg")
    half_width = w_out.shape[1] // 2
    w_half = lax.dynamic_slice_in_dim(w_out, cfg_index * half_width, half_width, 1)
    gate_half = lax.dynamic_slice_in_dim(gate, cfg_index * half_width, half_width, 1)
    partner = swapped(attended, "cfg", 0)
    own_update = gate_half * jnp.dot(attended, w_half, preferred_element_type=jnp.float32)
    other_update = gate_half * jnp.dot(partner, w_half, preferred_element_type=jnp.float32)
    is_first = cfg_index == 0
    cond = jnp.where(is_first, own_update, other_update)
    uncond = jnp.where(is_first, other_update, own_update)
    return uncond + GUIDANCE * (cond - uncond)


LANES = 128
GROUPS = 4
MESH = pl.DeviceIdType.MESH


def flip(bit, other):
    return lax.rem(bit + other, 2)


def pair_normal(x, low):
    def halves(y):
        first = jnp.sum(jnp.where(low, y, 0.0), axis=-1, keepdims=True)
        second = jnp.sum(jnp.where(low, 0.0, y), axis=-1, keepdims=True)
        return jnp.where(low, first, second) * (1.0 / HEAD)

    centred = x - halves(x)
    return centred * lax.rsqrt(halves(centred * centred) + EPSILON)


def turned(x):
    return pltpu.roll(x, HEAD, 1)


def fused(n, count_ref, block_ref, hidden_ref, mod_ref, w_ref, qg_ref, kg_ref, wo_ref, out_ref,
          w_buf, wo_buf, modded, kv_out, kv_in, q_out, q_in, bias_out, bias_in, bias_row,
          att_out, att_in, att_far, stacked,
          w_sem, wo_sem, kv_s, kv_r, q_s, q_r, b_s, b_r, a_s, a_r, f_s, f_r):
    me = lax.axis_index("seq")
    cfg = lax.axis_index("cfg")
    rows, width = hidden_ref.shape
    half_rows = rows // 2
    half = width // 2
    wide = wo_buf.shape[1]
    cols = w_buf.shape[3]
    heads_here = cols // HEAD
    plane = lax.div(me, GROUPS)
    plane_high, plane_low = lax.div(plane, 2), lax.rem(plane, 2)

    def group(i):
        high = 1 - lax.div(i, 2)
        lowbit = flip(lax.div(i, 2), lax.rem(i, 2))
        return 2 * flip(plane_high, high) + flip(plane_low, lowbit)

    def weight(kind, i):
        start = pl.multiple_of(group(i) * cols, cols)
        return pltpu.make_async_copy(
            w_ref.at[kind, :, pl.ds(start, cols)], w_buf.at[kind, i], w_sem.at[kind, i])

    column = pl.multiple_of(cfg * (width - wide), LANES)
    out_weight = pltpu.make_async_copy(wo_ref.at[:, pl.ds(column, wide)], wo_buf, wo_sem)

    barrier = pltpu.get_barrier_semaphore()
    for j in range(1, n):
        pl.semaphore_signal(barrier, inc=1, device_id={"seq": lax.rem(me + j, n)}, device_id_type=MESH)
    pl.semaphore_signal(barrier, inc=1, device_id={"cfg": 1 - cfg}, device_id_type=MESH)
    for i in range(GROUPS):
        weight(1, i).start()
        weight(2, i).start()
    for i in range(GROUPS):
        weight(0, i).start()
    out_weight.start()

    def send(src, dst, to, s_sem, r_sem):
        @pl.when(to != me)
        def _():
            pltpu.make_async_remote_copy(
                src_ref=src.at[to], dst_ref=dst.at[me], send_sem=s_sem.at[to], recv_sem=r_sem.at[me],
                device_id={"seq": to}, device_id_type=MESH).start()

        @pl.when(to == me)
        def _():
            pltpu.make_async_copy(src.at[to], dst.at[me], r_sem.at[me]).start()

    def arrived(dst, source, r_sem):
        pltpu.make_async_copy(dst.at[source], dst.at[source], r_sem.at[source]).wait()

    def sent(src, to, s_sem):
        @pl.when(to != me)
        def _():
            pltpu.make_async_copy(src.at[to], src.at[to], s_sem.at[to]).wait()

    block = block_ref[0]
    count = count_ref[0]
    across = block * rows + lax.broadcasted_iota(jnp.int32, (1, rows), 1)
    keep = jnp.logical_or(across >= TXT, across < count)
    bias_out[0:n] = jnp.broadcast_to(jnp.where(keep, 0.0, MASKED)[None], (n, 1, rows)).astype(jnp.bfloat16).astype(jnp.float32)

    mod = mod_ref[...]
    down = block * rows + lax.broadcasted_iota(jnp.int32, (rows, 1), 0)
    is_text = down < TXT
    normed = layer_normal(hidden_ref[...].astype(jnp.float32))
    shift = jnp.where(is_text, mod[3:4, :], mod[0:1, :])
    scale = jnp.where(is_text, mod[4:5, :], mod[1:2, :])
    modded[...] = (normed * (1.0 + scale) + shift).astype(jnp.bfloat16)

    low = lax.broadcasted_iota(jnp.int32, (1, LANES), 1) < HEAD
    pl.semaphore_wait(barrier, n)

    def send_bias(j, carry):
        send(bias_out, bias_in, j, b_s, b_r)
        return carry

    lax.fori_loop(0, n, send_bias, 0)

    k_gain = kg_ref[...]
    q_gain = qg_ref[...] * HEAD ** (-0.5)

    def project_kv(i, carry):
        weight(1, i).wait()
        weight(2, i).wait()
        first = group(i) * heads_here
        x = modded[...]
        k_all = jnp.dot(x, w_buf[1, i], preferred_element_type=jnp.float32)
        v_all = jnp.dot(x, w_buf[2, i], preferred_element_type=jnp.float32)
        for p in range(heads_here // 2):
            k = pair_normal(k_all[:, p * LANES:(p + 1) * LANES], low) * k_gain
            v = v_all[:, p * LANES:(p + 1) * LANES]
            kv_out[first + 2 * p] = jnp.where(low, k, turned(v)).astype(jnp.bfloat16)
            kv_out[first + 2 * p + 1] = jnp.where(low, turned(k), v).astype(jnp.bfloat16)
        for h in range(heads_here):
            send(kv_out, kv_in, first + h, kv_s, kv_r)
        return carry

    lax.fori_loop(0, GROUPS, project_kv, 0)

    def project_q(i, carry):
        weight(0, i).wait()
        first = group(i) * heads_here
        q_all = jnp.dot(modded[...], w_buf[0, i], preferred_element_type=jnp.float32)
        for p in range(heads_here // 2):
            q = pair_normal(q_all[:, p * LANES:(p + 1) * LANES], low) * q_gain
            top, bottom = q[:half_rows], q[half_rows:]
            q_out[first + 2 * p] = jnp.where(low, top, turned(bottom)).astype(jnp.bfloat16)
            q_out[first + 2 * p + 1] = jnp.where(low, turned(top), bottom).astype(jnp.bfloat16)
        for h in range(heads_here):
            send(q_out, q_in, first + h, q_s, q_r)
        return carry

    lax.fori_loop(0, GROUPS, project_q, 0)

    for j in range(n):
        arrived(bias_in, j, b_r)
    for j in range(n):
        bias_row[:, j * rows:(j + 1) * rows] = jnp.broadcast_to(bias_in[j], (8, rows))

    def wait_kv(j, carry):
        arrived(kv_in, j, kv_r)
        return carry

    lax.fori_loop(0, n, wait_kv, 0)

    chip = lax.div(me, 2)

    def pair_of(step):
        k = n // 2 - 1 - step
        c0, c1, c2 = lax.rem(chip, 2), lax.rem(lax.div(chip, 2), 2), lax.div(chip, 4)
        k0, k1, k2 = lax.rem(k, 2), lax.rem(lax.div(k, 2), 2), lax.div(k, 4)
        return 4 * flip(c2, k2) + 2 * flip(c1, k1) + flip(c0, k0)

    def forward(k):
        for i in range(2):
            h = 2 * pair_of(k) + i
            arrived(att_in, h, a_r)
            pltpu.make_async_remote_copy(
                src_ref=att_in.at[h], dst_ref=att_far.at[h], send_sem=f_s.at[h], recv_sem=f_r.at[h],
                device_id={"cfg": 1 - cfg}, device_id_type=MESH).start()

    def attend(k, carry):
        base = 2 * pair_of(k)
        parts = []
        for i in range(2):
            arrived(q_in, base + i, q_r)
            folded = q_in[base + i].astype(jnp.float32)
            parts += [jnp.where(low, folded, 0.0), jnp.where(low, turned(folded), 0.0)]
        keys = kv_in[...].reshape(n * rows, LANES)
        span = n * rows // 4
        done = []
        for g in range(1):
            piece = parts[g * (4 // 1):(g + 1) * (4 // 1)]
            query = jnp.concatenate(piece, axis=0).astype(jnp.bfloat16)
            scores = [
                lax.dot_general(query, keys[c * span:(c + 1) * span], (((1,), (1,)), ((), ())),
                                preferred_element_type=jnp.float32) + bias_row[0:1, c * span:(c + 1) * span]
                for c in range(4)
            ]
            highest = functools.reduce(jnp.maximum, [jnp.max(x, axis=-1, keepdims=True) for x in scores])
            total, numer = 0.0, 0.0
            for c in range(4):
                expo = jnp.exp(scores[c] - highest)
                total = total + jnp.sum(expo, axis=-1, keepdims=True)
                numer = numer + jnp.dot(expo.astype(jnp.bfloat16), keys[c * span:(c + 1) * span],
                                        preferred_element_type=jnp.float32)
            done.append(numer / total)
        result = jnp.concatenate(done, axis=0)
        for i in range(2):
            top = result[i * rows:i * rows + half_rows]
            bottom = result[i * rows + half_rows:(i + 1) * rows]
            att_out[base + i] = jnp.where(low, turned(top), bottom).astype(jnp.bfloat16)
            send(att_out, att_in, base + i, a_s, a_r)

        @pl.when(k >= 2)
        def _():
            forward(k - 2)

        return carry

    steps = n // 2
    lax.fori_loop(0, steps, attend, 0)
    forward(steps - 2)
    forward(steps - 1)
    out_weight.wait()

    def assemble(source, at):
        for p in range(n // 2):
            a = source[2 * p].astype(jnp.float32)
            b = source[2 * p + 1].astype(jnp.float32)
            span = slice(p * LANES, (p + 1) * LANES)
            stacked[at:at + half_rows, span] = jnp.where(low, a, turned(b)).astype(jnp.bfloat16)
            stacked[at + half_rows:at + rows, span] = jnp.where(low, turned(a), b).astype(jnp.bfloat16)

    assemble(att_in, 0)
    for h in range(n):
        arrived(att_far, h, f_r)
    assemble(att_far, rows)
    both = jnp.dot(stacked[...], wo_buf[...], preferred_element_type=jnp.float32)
    is_first = cfg == 0
    gate_text = jnp.where(is_first, mod[5:6, :wide], mod[5:6, width - wide:])
    gate_video = jnp.where(is_first, mod[2:3, :wide], mod[2:3, width - wide:])
    gate = jnp.where(is_text, gate_text, gate_video)
    own, other = gate * both[:rows], gate * both[rows:]
    cond = jnp.where(is_first, own, other)
    uncond = jnp.where(is_first, other, own)
    guided = uncond + GUIDANCE * (cond - uncond)
    excess = wide - half
    guided = jnp.where(is_first, guided, pltpu.roll(guided, half, 1)) if excess else guided
    out_ref[...] = guided[:, :half]

    def finish(j, carry):
        sent(bias_out, j, b_s)
        sent(kv_out, j, kv_s)
        sent(q_out, j, q_s)
        sent(att_out, j, a_s)
        pltpu.make_async_copy(att_in.at[j], att_in.at[j], f_s.at[j]).wait()
        return carry

    lax.fori_loop(0, n, finish, 0)


def whole_kernel(hidden, modulation, w_qkv, q_gain, k_gain, w_out, text_count, block_order):
    n = lax.axis_size("seq")
    states = hidden[0]
    rows, width = states.shape
    features = w_out.shape[0]
    cols = features // GROUPS
    half = width // 2
    wide = -(-half // LANES) * LANES
    bf, f32 = jnp.bfloat16, jnp.float32
    vmem = pl.BlockSpec(memory_space=pltpu.VMEM)
    smem = pl.BlockSpec(memory_space=pltpu.SMEM)
    hbm = pl.BlockSpec(memory_space=pl.ANY)
    dma = pltpu.SemaphoreType.DMA
    double = lambda gain: jnp.concatenate([gain, gain])[None, :]
    return pl.pallas_call(
        functools.partial(fused, n),
        out_shape=jax.ShapeDtypeStruct((rows, half), f32),
        in_specs=[smem, smem, vmem, vmem, hbm, vmem, vmem, hbm],
        out_specs=vmem,
        scratch_shapes=[
            pltpu.VMEM((3, GROUPS, width, cols), bf),
            pltpu.VMEM((features, wide), bf),
            pltpu.VMEM((rows, width), bf),
            pltpu.VMEM((n, rows, LANES), bf),
            pltpu.VMEM((n, rows, LANES), bf),
            pltpu.VMEM((n, rows // 2, LANES), bf),
            pltpu.VMEM((n, rows // 2, LANES), bf),
            pltpu.VMEM((n + 8, 1, rows), f32),
            pltpu.VMEM((n + 8, 1, rows), f32),
            pltpu.VMEM((8, n * rows), f32),
            pltpu.VMEM((n, rows // 2, LANES), bf),
            pltpu.VMEM((n, rows // 2, LANES), bf),
            pltpu.VMEM((n, rows // 2, LANES), bf),
            pltpu.VMEM((2 * rows, features), bf),
            dma((3, GROUPS)),
            dma,
        ] + [dma((n,))] * 10,
        compiler_params=pltpu.CompilerParams(
            collective_id=0, has_side_effects=True, vmem_limit_bytes=60 * 1024 * 1024),
    )(text_count, block_order, states, modulation, w_qkv, double(q_gain), double(k_gain), w_out)


def solution(mesh):
    in_specs = (P("cfg", "seq", None), P(), P(), P(), P(), P(), P("cfg"), P("seq"))
    out_specs = P("seq", "cfg")
    one_head_each = mesh.shape["seq"] == HEADS and mesh.shape["cfg"] == 2
    body = whole_kernel if one_head_each else shards
    return jax.shard_map(body, mesh=mesh, in_specs=in_specs, out_specs=out_specs, check_vma=False)
```
